32 devices in a mesh: real: 2 (over y), env: 4 (over z), mpo: 2 (over x), col: 2 (over core).
Axes of the slice: x: 2, y: 2, z: 4, core: 2. Of those that a mesh axis runs over, the one named last changes fastest.
Arguments:
- held: bfloat16 [3072, 8, 384], P(('real', 'env', 'col')), parts along dimension 0, may hold values from -0.15625 to 0.15625
- owner_map: int32 [8, 192], P('real'), parts along dimension 0, may hold values from 0 to 1535, as said below
- kept: int32 [8], P(('real', 'env')), parts along dimension 0, may hold values from 96 to 384
- left_env: bfloat16 [14, 8, 384, 384], P('mpo', ('real', 'env')), parts along dimension 1, may hold values from -6 to 6
- mpo_tensor: float32 [14, 14, 4, 4], replicated, may hold values from -1 to 1
- mpo_mask: int32 [14, 14], replicated, may hold values 0 or 1
- fields: float32 [4], P('real'), parts along dimension 0, may hold values from -2 to 2
Outputs:
- new_env: float32 [14, 8, 384, 384], P('mpo', ('real', 'env'), None, 'col'), parts along dimension 1
The draws below stay inside these ranges and needn't reach their ends.
There are 2 independent parts, one for each index of `real`. The reference program is written for one: setup_inputs(seed, part) draws one part's arguments, and reference() takes and returns one part's arrays. A program takes and returns all parts, laid end to end along the dimension named above; an argument that names none is the same for every part. Nothing has to cross between parts.
Inputs may be any that keep to these rules, and one draw needn't show every extreme that they name: owner_map[t, j] is the slot of held that holds tile j of sector t; all entries differ. The owner of index o along env+col holds the slots o * 192 to (o + 1) * 192 - 1. Among the tiles of one sector (the sector of one env index), one owner holds at most 48, and for every sector some owner holds exactly 48.
All inputs are finite; a program needn't handle non-finite values.
Results may differ from the reference program's by a relative error of at most 0.0042.
Values may be sent and summed in bfloat16 or wider, within the bound.
A program may use at most 64 MiB of HBM per device.

```python
import jax
import jax.numpy as jnp
from jax import lax

P_SIZE = 4
K = 14
B = 384
TILE = 8
SEC_DEV = 1
S = 4
NT = 192
CAP = 48
POOL = 192
SLOTS = 1536
KSL = 7
KP = 14
N_MPO = 2


def draw_owner_map(key, part):
    owners = 2 * SEC_DEV * NT // CAP
    row_count = S // SEC_DEV
    tiles_row = SEC_DEV * NT
    heavy = jax.random.randint(jax.random.fold_in(key, 11), (owners,), 0, 4)
    order = jax.vmap(lambda sub: jax.random.permutation(sub, POOL))(jax.random.split(jax.random.fold_in(key, 12), owners))

    def one_row(row):
        row_key = jax.random.fold_in(jax.random.fold_in(key, 13), row)
        candidate = jnp.arange(owners * CAP, dtype=jnp.int32)
        cand_owner = candidate // CAP
        noise = jax.random.randint(jax.random.fold_in(row_key, 1), (owners * CAP,), 0, 4096)
        forced = jax.random.randint(jax.random.fold_in(row_key, 2), (), 0, owners)
        score = noise + heavy[cand_owner] * 2048 + jnp.where(cand_owner == forced, 32768, 0)
        score = score * (owners * CAP) + candidate
        unused, chosen = lax.top_k(score, tiles_row)
        chosen = jax.random.permutation(jax.random.fold_in(row_key, 3), chosen)
        chosen_owner = chosen // CAP
        chosen_rank = chosen % CAP
        position = order[chosen_owner, row * CAP + chosen_rank]
        return chosen_owner * POOL + position
    table = jax.vmap(one_row)(jnp.arange(row_count, dtype=jnp.int32))
    return table.reshape(S, NT).astype(jnp.int32)


def with_ends(drawn, key, least, largest):
    longest = drawn.shape.index(max(drawn.shape))
    spots = []
    for shift in (0, 1):
        where = [jax.random.randint(jax.random.fold_in(key, axis), (), 0, length) for axis, length in enumerate(drawn.shape)]
        where[longest] = (where[longest] + shift) % drawn.shape[longest]
        spots.append(tuple(where))
    return drawn.at[spots[0]].set(least).at[spots[1]].set(largest)


def block_scale(stream_key, shape, shards, smallest, top_value):
    factor_of = 1.0
    for axis_at, blocks in shards:
        steps = jax.random.uniform(jax.random.fold_in(jax.random.fold_in(stream_key, 6), axis_at), (blocks,), jnp.float32, smallest / len(shards), top_value / len(shards))
        factor_of = factor_of * jnp.repeat(jnp.exp(steps), shape[axis_at] // blocks).reshape((-1,) + (1,) * (len(shape) - 1 - axis_at))
    return factor_of


def bell_draw(own_key, dims, width, limit, pieces=(), held_as=jnp.bfloat16):
    drawn = width * jax.random.normal(own_key, dims, jnp.float32)
    if pieces:
        drawn = drawn * block_scale(own_key, dims, pieces, -0.22, 0.18)
    return jnp.clip(drawn, -limit, limit).astype(held_as)


def setup_inputs(seed: int = 0, part: int = 0) -> dict:
    splits = jax.random.split(jax.random.key(seed), 8)
    own_keys = jax.random.split(jax.random.fold_in(splits[7], part), 8)
    return {
        "held": bell_draw(own_keys[0], (SLOTS, TILE, B), (P_SIZE * B) ** -0.5, 0.15625, ((0, 8),)),
        "owner_map": draw_owner_map(jax.random.fold_in(jax.random.fold_in(splits[7], part), 71), part),
        "kept": with_ends(jax.random.randint(own_keys[2], (S,), B // 4, B + 1), jax.random.fold_in(own_keys[2], 1), B // 4, B).astype(jnp.int32),
        "left_env": bell_draw(own_keys[3], (KP, S, B, B), 1.0, 6.0, ((0, 2), (1, 4))),
        "mpo_tensor": bell_draw(splits[4], (K, K, P_SIZE, P_SIZE), (K * P_SIZE // 2) ** -0.5, 1.0, (), jnp.float32),
        "mpo_mask": with_ends((jax.random.randint(splits[5], (K, K), 0, 2) < 1).astype(jnp.int32), jax.random.fold_in(splits[5], 1), 0, 1),
        "fields": jnp.clip(jax.random.uniform(own_keys[6], (2,), jnp.float32, -2.0, 2.0), -2.0, 2.0),
    }


def build_couplings(mpo_tensor, mpo_mask, fields, padded):
    bond = mpo_tensor.shape[0]
    states = mpo_tensor.shape[2]
    base = mpo_tensor * mpo_mask.astype(jnp.float32)[:, :, None, None]
    level = jnp.arange(states, dtype=jnp.int32)
    spin_first = 0.5 - (level // 2).astype(jnp.float32)
    spin_second = 0.5 - (level % 2).astype(jnp.float32)
    onsite = jnp.diag(fields[0] * spin_first + fields[1] * spin_second)
    bond_index = jnp.arange(bond, dtype=jnp.int32)
    corner = (bond_index[:, None] == bond - 1) & (bond_index[None, :] == 0)
    base = base + jnp.where(corner[:, :, None, None], onsite[None, None, :, :], jnp.float32(0.0))
    return jnp.pad(base, ((0, padded - bond), (0, padded - bond), (0, 0), (0, 0)))


def reference(held, owner_map, kept, left_env, mpo_tensor, mpo_mask, fields):
    tiles = jnp.take(held, owner_map.reshape(-1), axis=0)
    sector_matrices = tiles.reshape(S, P_SIZE, B, B)
    columns = jnp.arange(B, dtype=jnp.int32)
    keep = columns[None, :] < kept[:, None]
    sector_matrices = jnp.where(keep[:, None, None, :], sector_matrices, jnp.zeros((), jnp.bfloat16))
    couplings = build_couplings(mpo_tensor, mpo_mask, fields, KP)
    leading_sector = lax.Precision.HIGHEST

    def one_sector(pair):
        block, environment = pair
        bond_vectors = block.astype(jnp.float32)
        first = jnp.einsum("wij,sja->wsia", environment[:K].astype(jnp.float32), bond_vectors, precision=leading_sector)
        contracted_sum = jnp.zeros((K, P_SIZE, B, B), jnp.float32)
        for slab_index in range(N_MPO):
            lower = slab_index * KSL
            upper = min(lower + KSL, K)
            if lower < K:
                next_spin = jnp.einsum("wvts,wsia->vtia", couplings[lower:upper, :K], first[lower:upper], precision=leading_sector)
                rounded = lax.optimization_barrier(next_spin.astype(jnp.bfloat16))
                contracted_sum = contracted_sum + rounded.astype(jnp.float32)
        updated_environment = jnp.einsum("hze,shzo->seo", bond_vectors, contracted_sum, precision=leading_sector)
        return jnp.pad(updated_environment, ((0, KP - K), (0, 0), (0, 0)))

    stacked = lax.map(one_sector, (sector_matrices, jnp.moveaxis(left_env, 1, 0)))
    return jnp.moveaxis(stacked, 0, 1)
```

```python
import functools

import jax
import jax.numpy as jnp
from jax import lax
from jax.experimental import pallas as pl
from jax.experimental.pallas import tpu as pltpu
from jax.sharding import PartitionSpec as P

MESH = pl.DeviceIdType.MESH
LANES = 128
GROUP = 4
STEP = 16
ROWS = 64
EARLY = 3
BF = jnp.bfloat16
F32 = jnp.float32


def iota(shape, dim):
    return lax.broadcasted_iota(jnp.int32, shape, dim)


def one_hot(condition):
    return jnp.where(condition, F32(1), F32(0)).astype(BF)


def mm(a, b):
    return jnp.dot(a, b, preferred_element_type=F32)


def mm_nt(a, b):
    return lax.dot_general(a, b, (((1,), (1,)), ((), ())), preferred_element_type=F32)


def partner(env, d):
    out = env
    bit = 1
    while bit <= d:
        if d & bit:
            out = out + bit * (1 - 2 * lax.rem(lax.div(env, jnp.int32(bit)), 2))
        bit *= 2
    return out


def tile_lists(map_ref, env, me, pool, owners, cap):
    rows, tiles = map_ref.shape
    table = map_ref[...]
    if rows < 8:
        table = jnp.concatenate([table] * (8 // rows), axis=0)
    local = (table - me * pool).astype(F32)
    mine = (local >= 0) & (local < pool)
    earlier = one_hot(iota((tiles, tiles), 0) < iota((tiles, tiles), 1))
    rank = mm(jnp.where(mine, F32(1), F32(0)).astype(BF), earlier)
    key = jnp.where(mine, rank, F32(-1))
    places = rows * cap
    spread = one_hot(
        lax.div(iota((places, table.shape[0]), 0), cap) == iota((places, table.shape[0]), 1)
    )
    place = lax.rem(iota((places, tiles), 0), cap).astype(F32)
    chosen = one_hot(mm(spread, key.astype(BF)) == place)
    send = mm_nt(jnp.where(mine, local, F32(0)).astype(BF), chosen)
    send = send.astype(jnp.int32)

    row = map_ref[pl.ds(env, 1), :].astype(F32)
    owner = jnp.floor((row + 0.5) * F32(1.0 / pool))
    holds = iota((owners, tiles), 0).astype(F32) == owner
    ranks = mm(one_hot(holds), earlier)
    at = owner * cap + jnp.sum(jnp.where(holds, ranks, F32(0)), axis=0, keepdims=True)
    return send, at.astype(jnp.int32)


def mixing_matrix(tensor_ref, mask_ref, fields_ref, table_ref, plane, slab, slots, padded):
    bond, states = tensor_ref.shape[0], tensor_ref.shape[1]
    table_ref[...] = jnp.zeros_like(table_ref)
    lane, state = iota((states, bond), 1), iota((states, bond), 0)
    onsite = fields_ref[0] * (0.5 - lax.div(state, 2).astype(F32)) + fields_ref[1] * (
        0.5 - lax.rem(state, 2).astype(F32)
    )
    for w in range(bond):
        mask = mask_ref[pl.ds(w, 1), :].astype(F32)
        for q in range(states):
            block = tensor_ref[w, q] * mask
            if w == bond - 1:
                block = block + jnp.where((lane == 0) & (state == q), onsite, F32(0))
            table_ref[pl.ds((w * states + q) * states, states), :bond] = block
    table = table_ref[...]
    high = table.astype(BF)
    low = (table - high.astype(F32)).astype(BF)

    wide, tall = states * GROUP * padded, slab * states * GROUP
    entries = table.shape[0]
    at, entry = iota((wide, entries), 0), iota((wide, entries), 1)
    slot = lax.rem(at, padded)
    bond_index = plane * slab + slot
    bond_index = jnp.where(bond_index >= slots, bond_index - slots, bond_index)
    base = bond_index * (states * states) + lax.div(at, GROUP * padded)
    row, col = iota((tall, LANES), 0), iota((tall, LANES), 1)
    unit = states * GROUP
    diagonal = lax.rem(iota((tall, wide), 0), GROUP) == lax.rem(
        lax.div(iota((tall, wide), 1), padded), GROUP
    )
    parts = [jnp.zeros((tall, wide), F32), jnp.zeros((tall, wide), F32)]
    for q in range(states):
        source = one_hot((entry == base + q * states) & (slot < slots))
        target = one_hot(
            (lax.div(lax.rem(row, unit), GROUP) == q) & (col == plane * slab + lax.div(row, unit))
        )
        for i, piece in enumerate((high, low)):
            parts[i] = parts[i] + mm_nt(target, mm(source, piece).astype(BF))
    return jnp.concatenate([jnp.where(diagonal, part, F32(0)).astype(BF) for part in parts], axis=0)


def fused_kernel(
    sizes, kept_ref, fields_ref, map_ref, tensor_ref, mask_ref, held_ref, left_ref,
    second_ref, turned_ref,
    pool_ref, pack_ref, arrived_ref, near_ref, far_ref, vlist_ref, list_ref, table_ref,
    tiles_ref, own_ref, first_ref,
    z_send, z_recv, f_send, f_recv, s_send, s_recv, t_send, t_recv,
    x_send, x_recv, g_send, g_recv, local_sem,
):
    envs, planes, cores = sizes
    env, plane, core = lax.axis_index("env"), lax.axis_index("mpo"), lax.axis_index("col")
    pool, tile, width = pool_ref.shape
    rows, tiles = map_ref.shape
    owners = envs * cores
    cap = pack_ref.shape[1]
    states = tiles * tile // width
    slab = left_ref.shape[0]
    slots = slab * planes
    padded = -(-slots // 16) * 16
    share = width // cores
    lanes = own_ref.shape[2]
    mate = lax.rem(core + 1, cores)
    me = env * cores + core
    chunks = width // ROWS
    part = ROWS // cores
    early = min(EARLY, chunks)
    half = cap // planes
    shared = [d >= envs // 2 and cap % planes == 0 for d in range(envs)]

    fill = pltpu.make_async_copy(held_ref, pool_ref, local_sem.at[0])
    fill.start()
    barrier = pltpu.get_barrier_semaphore()
    for d in range(1, envs):
        pl.semaphore_signal(
            barrier, inc=1, device_id={"env": partner(env, d)}, device_id_type=MESH
        )
    for d in range(1, planes):
        pl.semaphore_signal(
            barrier, inc=1, device_id={"mpo": lax.rem(plane + d, planes)}, device_id_type=MESH
        )
    pl.semaphore_signal(barrier, inc=1, device_id={"col": mate}, device_id_type=MESH)

    send, at = tile_lists(map_ref, env, me, pool, owners, cap)
    send_rows = send.shape[0]
    vlist_ref[:send_rows] = send
    vlist_ref[pl.ds(send_rows, 8)] = jnp.broadcast_to(at, (8, tiles))
    lists = pltpu.make_async_copy(vlist_ref, list_ref, local_sem.at[1])
    lists.start()
    near = pltpu.make_async_copy(left_ref, near_ref, local_sem.at[2])
    near.start()
    pl.semaphore_wait(barrier, envs + planes - 1)

    def span(d, owner_plane):
        return (owner_plane * half, half) if shared[d] else (0, cap)

    def z_copy(d):
        start, count = span(d, plane)
        return pltpu.make_async_remote_copy(
            src_ref=pack_ref.at[d - 1, pl.ds(0, count)],
            dst_ref=arrived_ref.at[pl.ds(me * cap + start, count)],
            send_sem=z_send.at[d], recv_sem=z_recv.at[d],
            device_id={"env": partner(env, d)}, device_id_type=MESH,
        )

    def landed(d, owner_plane):
        start, count = (0, cap) if d == 0 else span(d, owner_plane)
        source = (partner(env, d) if d else env) * cores + core
        return arrived_ref.at[pl.ds(source * cap + start, count)]

    def f_copy(d):
        return pltpu.make_async_remote_copy(
            src_ref=landed(d, plane), dst_ref=landed(d, plane),
            send_sem=f_send.at[d], recv_sem=f_recv.at[d],
            device_id={"col": mate}, device_id_type=MESH,
        )

    def s_copy(d, e):
        return pltpu.make_async_remote_copy(
            src_ref=landed(d, plane), dst_ref=landed(d, plane),
            send_sem=s_send.at[d, e], recv_sem=s_recv.at[d, e],
            device_id={"mpo": lax.rem(plane + e, planes)}, device_id_type=MESH,
        )

    def t_copy(d, e):
        block = landed(d, lax.rem(plane + planes - e, planes))
        return pltpu.make_async_remote_copy(
            src_ref=block, dst_ref=block,
            send_sem=t_send.at[d, e], recv_sem=t_recv.at[d, e],
            device_id={"col": mate}, device_id_type=MESH,
        )

    def x_copy(d, h):
        piece = pl.ds(pl.multiple_of(h * ROWS + core * part, part), part)
        return pltpu.make_async_remote_copy(
            src_ref=left_ref.at[:, 0, piece],
            dst_ref=far_ref.at[pl.ds((planes - d - 1) * slab, slab), piece],
            send_sem=x_send.at[d, h], recv_sem=x_recv.at[d, h],
            device_id={"mpo": lax.rem(plane + d, planes)}, device_id_type=MESH,
        )

    def g_copy(d, h):
        piece = pl.ds(pl.multiple_of(h * ROWS + core * part, part), part)
        block = far_ref.at[pl.ds((planes - d - 1) * slab, slab), piece]
        return pltpu.make_async_remote_copy(
            src_ref=block, dst_ref=block,
            send_sem=g_send.at[d, h], recv_sem=g_recv.at[d, h],
            device_id={"col": mate}, device_id_type=MESH,
        )

    def x_start(h):
        for d in range(1, planes):
            x_copy(d, h).start()

    def x_pass(h):
        for d in range(1, planes):
            x_copy(d, h).wait_recv()
            g_copy(d, h).start()

    for h in range(early):
        x_start(h)
    fill.wait()
    lists.wait()

    def gather(count, slot_at, store):
        def step(p, carry):
            store(p, pool_ref[jnp.clip(slot_at(p), 0, pool - 1)])
            return carry

        lax.fori_loop(0, count, step, jnp.int32(0), unroll=8 if count % 8 == 0 else 1)

    z_order = list(range(envs - 1, 0, -1))
    for d in z_order:
        target = partner(env, d)
        start, count = span(d, plane)

        def store(p, value, d=d):
            pack_ref[d - 1, p] = value

        gather(count, lambda p: list_ref[target, target * cap + start + p], store)
        z_copy(d).start()

    def keep(p, value):
        arrived_ref[me * cap + p] = value

    gather(cap, lambda p: list_ref[env, env * cap + p], keep)
    f_copy(0).start()

    mixing = mixing_matrix(
        tensor_ref, mask_ref, fields_ref, table_ref, plane, slab, slots, padded
    )

    for d in z_order:
        z_copy(d).wait_recv()
        if shared[d]:
            for e in range(1, planes):
                s_copy(d, e).start()
        f_copy(d).start()
    for h in range(early, chunks):
        x_start(h)
    for h in range(early):
        x_pass(h)
    for d in z_order:
        if shared[d]:
            for e in range(1, planes):
                s_copy(d, e).wait_recv()
                t_copy(d, e).start()
    for d in range(envs):
        f_copy(d).wait_recv()
    for d in z_order:
        if shared[d]:
            for e in range(1, planes):
                t_copy(d, e).wait_recv()

    batch = 16 if tiles % 16 == 0 else 1

    def fetch(b, carry):
        for i in range(batch):
            j = b * batch + i
            to = pl.multiple_of(j * tile, tile)
            source = jnp.clip(list_ref[send_rows, j], 0, owners * cap - 1)
            tiles_ref[pl.ds(to, tile), :] = arrived_ref[source].astype(F32)
        return carry

    lax.fori_loop(0, tiles // batch, fetch, jnp.int32(0))

    kept = kept_ref[0]
    blocks = [
        jnp.where(
            iota((width, width), 1) < kept, tiles_ref[pl.ds(s * width, width), :], F32(0)
        ).astype(BF)
        for s in range(states)
    ]
    pick = one_hot(
        (iota((width, lanes), 0) == iota((width, lanes), 1) + core * share)
        & (iota((width, lanes), 1) < share)
    )
    for s in range(states):
        own_ref[s] = mm(blocks[s], pick).astype(BF)

    chunk = 256 // states
    wide = chunk * states
    row, col = iota((wide, wide), 0), iota((wide, wide), 1)
    unit = states * GROUP
    moved = (
        lax.rem(lax.div(row, GROUP), states) * chunk
        + lax.div(row, unit) * GROUP
        + lax.rem(row, GROUP)
    )
    regroup = one_hot(col == moved)
    for h in range(width // chunk):
        stack = jnp.concatenate(
            [blocks[s][h * chunk : (h + 1) * chunk] for s in range(states)], axis=0
        )
        turned_ref[:, pl.ds(h * wide, wide)] = mm(regroup, stack).T.astype(BF)

    block_rows = STEP * padded
    row, col = iota((block_rows, block_rows), 0), iota((block_rows, block_rows), 1)
    interleave = one_hot(col == lax.rem(row, padded) * STEP + lax.div(row, padded))
    per_group = GROUP * padded
    tall = slab * states * GROUP

    def chunk_step(h, carry):
        @pl.when(h >= early)
        def _():
            x_pass(h)

        for d in range(1, planes):
            g_copy(d, h).wait_recv()
        pieces = []
        for b in range(ROWS // STEP):
            piece = pl.ds(pl.multiple_of(h * ROWS + b * STEP, STEP), STEP)
            stack = [near_ref[w, 0, piece, :] for w in range(slab)]
            stack += [far_ref[w, piece, :] for w in range(slots - slab)]
            if padded > slots:
                stack.append(jnp.zeros(((padded - slots) * STEP, width), BF))
            pieces.append(mm(interleave, jnp.concatenate(stack, axis=0)).astype(BF))
        environment = jnp.concatenate(pieces, axis=0)
        for s in range(states):
            first_ref[s] = mm(environment, own_ref[s]).astype(BF)
        for g in range(ROWS // GROUP):
            operand = jnp.concatenate(
                [first_ref[s, pl.ds(g * per_group, per_group), :] for s in range(states)], axis=0
            )
            mixed = mm(mixing, operand)
            mixed = (mixed[:tall] + mixed[tall:]).astype(BF)
            to = pl.multiple_of(h * (ROWS * states) + g * unit, unit)
            for v in range(slab):
                second_ref[v, pl.ds(to, unit), :] = mixed[v * unit : (v + 1) * unit]
        return carry

    near.wait()
    lax.fori_loop(0, chunks, chunk_step, jnp.int32(0))

    for d in range(envs):
        if d:
            z_copy(d).wait_send()
        f_copy(d).wait_send()
        if shared[d]:
            for e in range(1, planes):
                s_copy(d, e).wait_send()
                t_copy(d, e).wait_send()

    def drain(h, carry):
        for d in range(1, planes):
            x_copy(d, h).wait_send()
            g_copy(d, h).wait_send()
        return carry

    lax.fori_loop(0, chunks, drain, jnp.int32(0))


def close_kernel(second_ref, turned_ref, out_ref):
    slab, share, _ = out_ref.shape

    def close(v, carry):
        out_ref[v] = mm(turned_ref[...], second_ref[v]).T[:share]
        return carry

    lax.fori_loop(0, slab, close, jnp.int32(0))


def on_device(held, owner_map, kept, left_env, mpo_tensor, mpo_mask, fields):
    envs, cores, planes = (lax.axis_size(name) for name in ("env", "col", "mpo"))
    pool, tile, width = held.shape
    rows, tiles = owner_map.shape
    states = tiles * tile // width
    cap = 2 * kept.shape[0] * tiles // (envs * cores)
    slab = left_env.shape[0]
    slots = slab * planes
    padded = -(-slots // 16) * 16
    share = width // cores
    lanes = -(-share // LANES) * LANES
    chunks = width // ROWS
    bond = mpo_tensor.shape[0]
    list_rows = max(rows, 8) + 8
    smem = pl.BlockSpec(memory_space=pltpu.SMEM)
    vmem = pl.BlockSpec(memory_space=pltpu.VMEM)
    anywhere = pl.BlockSpec(memory_space=pl.ANY)
    dma = pltpu.SemaphoreType.DMA
    assert pool <= 256 and envs & (envs - 1) == 0 and kept.shape[0] == 1

    second, turned = pl.pallas_call(
        functools.partial(fused_kernel, (envs, planes, cores)),
        out_shape=[
            jax.ShapeDtypeStruct((slab, tiles * tile, lanes), BF),
            jax.ShapeDtypeStruct((width, tiles * tile), BF),
        ],
        in_specs=[smem, smem, vmem, vmem, vmem, anywhere, anywhere],
        out_specs=[vmem, vmem],
        scratch_shapes=[
            pltpu.VMEM((pool, tile, width), BF),
            pltpu.VMEM((max(envs - 1, 1), cap, tile, width), BF),
            pltpu.VMEM((envs * cores * cap, tile, width), BF),
            pltpu.VMEM(left_env.shape, BF),
            pltpu.VMEM((slots - slab, width, width), BF),
            pltpu.VMEM((list_rows, tiles), jnp.int32),
            pltpu.SMEM((list_rows, tiles), jnp.int32),
            pltpu.VMEM((bond * states * states, LANES), F32),
            pltpu.VMEM((tiles * tile, width), F32),
            pltpu.VMEM((states, width, lanes), BF),
            pltpu.VMEM((states, ROWS * padded, lanes), BF),
            dma((envs,)), dma((envs,)), dma((envs,)), dma((envs,)),
            dma((envs, planes)), dma((envs, planes)), dma((envs, planes)), dma((envs, planes)),
            dma((planes, chunks)), dma((planes, chunks)),
            dma((planes, chunks)), dma((planes, chunks)),
            dma((3,)),
        ],
        compiler_params=pltpu.CompilerParams(
            collective_id=0, has_side_effects=True, vmem_limit_bytes=62 * 1024 * 1024
        ),
        name="fused",
    )(kept, fields, owner_map, mpo_tensor.transpose(0, 2, 3, 1), mpo_mask, held, left_env)

    result = pl.pallas_call(
        close_kernel,
        out_shape=jax.ShapeDtypeStruct((slab, share, width), F32),
        in_specs=[vmem, vmem],
        out_specs=vmem,
        compiler_params=pltpu.CompilerParams(vmem_limit_bytes=62 * 1024 * 1024),
        name="close",
    )(second, turned)
    return jnp.swapaxes(result, 1, 2)[:, None]


def solution(mesh):
    return jax.shard_map(
        on_device,
        mesh=mesh,
        in_specs=(
            P(("real", "env", "col"), None, None),
            P("real", None),
            P(("real", "env")),
            P("mpo", ("real", "env"), None, None),
            P(),
            P(),
            P("real"),
        ),
        out_specs=P("mpo", ("real", "env"), None, "col"),
        check_vma=False,
    )
```

```python
import functools

import jax
import jax.numpy as jnp
from jax import lax
from jax.experimental import pallas as pl
from jax.experimental.pallas import tpu as pltpu
from jax.sharding import PartitionSpec as P

MESH = pl.DeviceIdType.MESH
LANES = 128
GROUP = 4
STEP = 16
ROWS = 64
EARLY = 2
MIDDLE = 1
WINDOW = 2
PIECES = 2
BF = jnp.bfloat16
F32 = jnp.float32


def iota(shape, dim):
    return lax.broadcasted_iota(jnp.int32, shape, dim)


def one_hot(condition):
    return jnp.where(condition, F32(1), F32(0)).astype(BF)


def mm(a, b):
    return jnp.dot(a, b, preferred_element_type=F32)


def mm_nt(a, b):
    return lax.dot_general(a, b, (((1,), (1,)), ((), ())), preferred_element_type=F32)


def mm_tn(a, b):
    return lax.dot_general(a, b, (((0,), (0,)), ((), ())), preferred_element_type=F32)


def partner(env, d):
    out = env
    bit = 1
    while bit <= d:
        if d & bit:
            out = out + bit * (1 - 2 * lax.rem(lax.div(env, jnp.int32(bit)), 2))
        bit *= 2
    return out


def tile_lists(map_ref, env, me, pool, owners, cap):
    rows, tiles = map_ref.shape
    table = map_ref[...]
    if rows < 8:
        table = jnp.concatenate([table] * (8 // rows), axis=0)
    local = (table - me * pool).astype(F32)
    mine = (local >= 0) & (local < pool)
    earlier = one_hot(iota((tiles, tiles), 0) < iota((tiles, tiles), 1))
    rank = mm(jnp.where(mine, F32(1), F32(0)).astype(BF), earlier)
    key = jnp.where(mine, rank, F32(-1))
    places = rows * cap
    spread = one_hot(
        lax.div(iota((places, table.shape[0]), 0), cap) == iota((places, table.shape[0]), 1)
    )
    place = lax.rem(iota((places, tiles), 0), cap).astype(F32)
    chosen = one_hot(mm(spread, key.astype(BF)) == place)
    send = mm_nt(jnp.where(mine, local, F32(0)).astype(BF), chosen)
    send = send.astype(jnp.int32)

    row = map_ref[pl.ds(env, 1), :].astype(F32)
    owner = jnp.floor((row + 0.5) * F32(1.0 / pool))
    holds = iota((owners, tiles), 0).astype(F32) == owner
    ranks = mm(one_hot(holds), earlier)
    at = owner * cap + jnp.sum(jnp.where(holds, ranks, F32(0)), axis=0, keepdims=True)
    return send, at.astype(jnp.int32)


def mixing_matrix(tensor_ref, mask_ref, fields_ref, table_ref, plane, slab, slots, padded):
    bond, states = tensor_ref.shape[0], tensor_ref.shape[1]
    table_ref[...] = jnp.zeros_like(table_ref)
    lane, state = iota((states, bond), 1), iota((states, bond), 0)
    onsite = fields_ref[0] * (0.5 - lax.div(state, 2).astype(F32)) + fields_ref[1] * (
        0.5 - lax.rem(state, 2).astype(F32)
    )
    for w in range(bond):
        mask = mask_ref[pl.ds(w, 1), :].astype(F32)
        for q in range(states):
            block = tensor_ref[w, q] * mask
            if w == bond - 1:
                block = block + jnp.where((lane == 0) & (state == q), onsite, F32(0))
            table_ref[pl.ds((w * states + q) * states, states), :bond] = block
    table = table_ref[...]
    high = table.astype(BF)
    low = (table - high.astype(F32)).astype(BF)

    wide, tall = states * GROUP * padded, slab * states * GROUP
    entries = table.shape[0]
    at, entry = iota((wide, entries), 0), iota((wide, entries), 1)
    slot = lax.rem(at, padded)
    bond_index = plane * slab + slot
    bond_index = jnp.where(bond_index >= slots, bond_index - slots, bond_index)
    base = bond_index * (states * states) + lax.div(at, GROUP * padded)
    row, col = iota((tall, LANES), 0), iota((tall, LANES), 1)
    unit = states * GROUP
    diagonal = lax.rem(iota((tall, wide), 0), GROUP) == lax.rem(
        lax.div(iota((tall, wide), 1), padded), GROUP
    )
    parts = [jnp.zeros((tall, wide), F32), jnp.zeros((tall, wide), F32)]
    for q in range(states):
        source = one_hot((entry == base + q * states) & (slot < slots))
        target = one_hot(
            (lax.div(lax.rem(row, unit), GROUP) == q) & (col == plane * slab + lax.div(row, unit))
        )
        for i, piece in enumerate((high, low)):
            parts[i] = parts[i] + mm_nt(target, mm(source, piece).astype(BF))
    return jnp.concatenate([jnp.where(diagonal, part, F32(0)).astype(BF) for part in parts], axis=0)


def fused_kernel(
    sizes, kept_ref, fields_ref, map_ref, tensor_ref, mask_ref, held_ref, left_ref,
    out_ref,
    pool_ref, pack_ref, arrived_ref, near_ref, far_ref, vlist_ref, list_ref, table_ref,
    tiles_ref, own_ref, first_ref, second_ref, close_ref, vmap_ref, vtensor_ref, vmask_ref,
    z_send, z_recv, f_send, f_recv, s_send, s_recv, t_send, t_recv,
    x_send, x_recv, g_send, g_recv, local_sem,
):
    envs, planes, cores = sizes
    env, plane, core = lax.axis_index("env"), lax.axis_index("mpo"), lax.axis_index("col")
    pool, tile, width = pool_ref.shape
    rows, tiles = map_ref.shape
    owners = envs * cores
    cap = pack_ref.shape[1]
    states = tiles * tile // width
    slab = left_ref.shape[0]
    slots = slab * planes
    padded = -(-slots // 16) * 16
    share = width // cores
    lanes = own_ref.shape[2]
    mate = lax.rem(core + 1, cores)
    me = env * cores + core
    chunks = width // ROWS
    part = ROWS // cores
    half = cap // planes
    pieces = PIECES if half % PIECES == 0 else 1
    shared = [d >= envs // 2 and cap % planes == 0 for d in range(envs)]
    order = range(envs - 1, 0, -1)
    cross = [(d, k) for d in order if shared[d] for k in range(pieces)]
    local = [(d, 0) for d in order if not shared[d]]
    passed = min(EARLY + MIDDLE, chunks)
    begun = min(passed + WINDOW, chunks)

    barrier = pltpu.get_barrier_semaphore()
    for d in range(1, planes):
        pl.semaphore_signal(
            barrier, inc=1, device_id={"mpo": lax.rem(plane + d, planes)}, device_id_type=MESH
        )
    pl.semaphore_signal(barrier, inc=1, device_id={"col": mate}, device_id_type=MESH)
    for d in range(1, envs):
        pl.semaphore_signal(
            barrier, inc=1, device_id={"env": partner(env, d)}, device_id_type=MESH
        )
    loads = [
        pltpu.make_async_copy(source, target, local_sem.at[i])
        for i, (source, target) in enumerate(
            [
                (map_ref, vmap_ref), (held_ref, pool_ref), (tensor_ref, vtensor_ref),
                (mask_ref, vmask_ref), (left_ref, near_ref), (vlist_ref, list_ref),
            ]
        )
    ]
    for load in loads[:5]:
        load.start()
    loads[0].wait()

    send, at = tile_lists(vmap_ref, env, me, pool, owners, cap)
    send_rows = send.shape[0]
    vlist_ref[:send_rows] = send
    vlist_ref[pl.ds(send_rows, 8)] = jnp.broadcast_to(at, (8, tiles))
    loads[5].start()

    def span(d, k, owner_plane):
        count = half // pieces
        return (owner_plane * half + k * count, count) if shared[d] else (0, cap)

    def landed(d, k, owner_plane):
        start, count = (0, cap) if d == 0 else span(d, k, owner_plane)
        source = (partner(env, d) if d else env) * cores + core
        return arrived_ref.at[pl.ds(source * cap + start, count)]

    def z_copy(d, k):
        start, count = span(d, k, plane)
        return pltpu.make_async_remote_copy(
            src_ref=pack_ref.at[d - 1, pl.ds(k * count, count)],
            dst_ref=arrived_ref.at[pl.ds(me * cap + start, count)],
            send_sem=z_send.at[d, k], recv_sem=z_recv.at[d, k],
            device_id={"env": partner(env, d)}, device_id_type=MESH,
        )

    def f_copy(d, k):
        block = landed(d, k, plane)
        return pltpu.make_async_remote_copy(
            src_ref=block, dst_ref=block,
            send_sem=f_send.at[d, k], recv_sem=f_recv.at[d, k],
            device_id={"col": mate}, device_id_type=MESH,
        )

    def s_copies(d, k):
        block = landed(d, k, plane)
        return [
            pltpu.make_async_remote_copy(
                src_ref=block, dst_ref=block,
                send_sem=s_send.at[d, k, e], recv_sem=s_recv.at[d, k, e],
                device_id={"mpo": lax.rem(plane + e, planes)}, device_id_type=MESH,
            )
            for e in range(1, planes)
        ]

    def t_copies(d, k):
        copies = []
        for e in range(1, planes):
            block = landed(d, k, lax.rem(plane + planes - e, planes))
            copies.append(
                pltpu.make_async_remote_copy(
                    src_ref=block, dst_ref=block,
                    send_sem=t_send.at[d, k, e], recv_sem=t_recv.at[d, k, e],
                    device_id={"col": mate}, device_id_type=MESH,
                )
            )
        return copies

    def x_copies(h):
        piece = pl.ds(pl.multiple_of(h * ROWS + core * part, part), part)
        return [
            pltpu.make_async_remote_copy(
                src_ref=left_ref.at[:, 0, piece],
                dst_ref=far_ref.at[pl.ds((planes - d - 1) * slab, slab), piece],
                send_sem=x_send.at[d, h], recv_sem=x_recv.at[d, h],
                device_id={"mpo": lax.rem(plane + d, planes)}, device_id_type=MESH,
            )
            for d in range(1, planes)
        ]

    def g_copies(h):
        piece = pl.ds(pl.multiple_of(h * ROWS + core * part, part), part)
        copies = []
        for d in range(1, planes):
            block = far_ref.at[pl.ds((planes - d - 1) * slab, slab), piece]
            copies.append(
                pltpu.make_async_remote_copy(
                    src_ref=block, dst_ref=block,
                    send_sem=g_send.at[d, h], recv_sem=g_recv.at[d, h],
                    device_id={"col": mate}, device_id_type=MESH,
                )
            )
        return copies

    def start(copies):
        for copy in copies:
            copy.start()

    def sent(copies):
        for copy in copies:
            copy.wait_send()

    def relay(arrivals, copies):
        for arrival, copy in zip(arrivals, copies):
            arrival.wait_recv()
            copy.start()

    pl.semaphore_wait(barrier, envs + planes - 1)
    for h in range(EARLY):
        start(x_copies(h))
    loads[1].wait()
    loads[5].wait()

    def gather(count, first, store):
        def step(p, carry):
            slot = jnp.clip(list_ref[first[0], first[1] + p], 0, pool - 1)
            store(p, pool_ref[slot])
            return carry

        lax.fori_loop(0, count, step, jnp.int32(0), unroll=8 if count % 8 == 0 else 4 if count % 4 == 0 else 1)

    def pack(d, k):
        target = partner(env, d)
        begin, count = span(d, k, plane)

        def store(p, value):
            pack_ref[d - 1, k * count + p] = value

        gather(count, (target, target * cap + begin), store)

    ahead = cross[:WINDOW] + local
    for item in ahead:
        pack(*item)
        z_copy(*item).start()
    for item in cross[WINDOW:]:
        pack(*item)

    def keep(p, value):
        arrived_ref[me * cap + p] = value

    gather(cap, (env, env * cap), keep)
    f_copy(0, 0).start()

    loads[2].wait()
    loads[3].wait()
    mixing = mixing_matrix(
        vtensor_ref, vmask_ref, fields_ref, table_ref, plane, slab, slots, padded
    )
    out_ref[...] = jnp.zeros_like(out_ref)

    for i, item in enumerate(cross):
        if i + WINDOW < len(cross):
            z_copy(*item).wait_send()
            z_copy(*cross[i + WINDOW]).start()
        z_copy(*item).wait_recv()
        start(s_copies(*item))
        f_copy(*item).start()
        if i == len(cross) // 2 - 1:
            for h in range(EARLY, passed):
                start(x_copies(h))
    if not cross:
        for h in range(EARLY, passed):
            start(x_copies(h))
    for item in local:
        z_copy(*item).wait_recv()
        f_copy(*item).start()
    for h in range(passed):
        relay(x_copies(h), g_copies(h))
    for item in cross:
        sent(s_copies(*item))
    for h in range(passed, begun):
        start(x_copies(h))
    for item in cross:
        relay(s_copies(*item), t_copies(*item))
    for d, k in [(0, 0)] + cross + local:
        f_copy(d, k).wait_recv()
    for item in cross:
        for copy in t_copies(*item):
            copy.wait_recv()

    batch = 16 if tiles % 16 == 0 else 1

    def fetch(b, carry):
        for i in range(batch):
            j = b * batch + i
            to = pl.multiple_of(j * tile, tile)
            source = jnp.clip(list_ref[send_rows, j], 0, owners * cap - 1)
            tiles_ref[pl.ds(to, tile), :] = arrived_ref[source].astype(F32)
        return carry

    lax.fori_loop(0, tiles // batch, fetch, jnp.int32(0))

    kept = kept_ref[0]
    blocks = [
        jnp.where(
            iota((width, width), 1) < kept, tiles_ref[pl.ds(s * width, width), :], F32(0)
        ).astype(BF)
        for s in range(states)
    ]
    pick = one_hot(
        (iota((width, lanes), 0) == iota((width, lanes), 1) + core * share)
        & (iota((width, lanes), 1) < share)
    )
    for s in range(states):
        own_ref[s] = mm(blocks[s], pick).astype(BF)

    wide = ROWS * states
    row, col = iota((wide, wide), 0), iota((wide, wide), 1)
    unit = states * GROUP
    moved = (
        lax.rem(lax.div(row, GROUP), states) * ROWS
        + lax.div(row, unit) * GROUP
        + lax.rem(row, GROUP)
    )
    regroup = one_hot(col == moved)
    for h in range(chunks):
        stack = jnp.concatenate(
            [blocks[s][h * ROWS : (h + 1) * ROWS] for s in range(states)], axis=0
        )
        close_ref[pl.ds(h * wide, wide), :] = mm(regroup, stack).astype(BF)

    block_rows = STEP * padded
    row, col = iota((block_rows, block_rows), 0), iota((block_rows, block_rows), 1)
    interleave = one_hot(col == lax.rem(row, padded) * STEP + lax.div(row, padded))
    per_group = GROUP * padded
    tall = slab * states * GROUP

    def chunk_step(h, carry):
        @pl.when(h + begun < chunks)
        def _():
            sent(x_copies(h + begun - WINDOW))
            start(x_copies(h + begun))

        @pl.when((h + 1 >= passed) & (h + 1 < chunks))
        def _():
            relay(x_copies(h + 1), g_copies(h + 1))

        for copy in g_copies(h):
            copy.wait_recv()
        parts = []
        for b in range(ROWS // STEP):
            piece = pl.ds(pl.multiple_of(h * ROWS + b * STEP, STEP), STEP)
            stack = [near_ref[w, 0, piece, :] for w in range(slab)]
            stack += [far_ref[w, piece, :] for w in range(slots - slab)]
            if padded > slots:
                stack.append(jnp.zeros(((padded - slots) * STEP, width), BF))
            parts.append(mm(interleave, jnp.concatenate(stack, axis=0)).astype(BF))
        environment = jnp.concatenate(parts, axis=0)
        for s in range(states):
            first_ref[s] = mm(environment, own_ref[s]).astype(BF)
        for g in range(ROWS // GROUP):
            operand = jnp.concatenate(
                [first_ref[s, pl.ds(g * per_group, per_group), :] for s in range(states)], axis=0
            )
            mixed = mm(mixing, operand)
            mixed = (mixed[:tall] + mixed[tall:]).astype(BF)
            for v in range(slab):
                second_ref[v, pl.ds(g * unit, unit), :] = mixed[v * unit : (v + 1) * unit]
        right = close_ref[pl.ds(pl.multiple_of(h * wide, wide), wide), :]
        for v in range(slab):
            out_ref[v] += mm_tn(second_ref[v], right)[:share]
        return carry

    loads[4].wait()
    lax.fori_loop(0, chunks, chunk_step, jnp.int32(0))

    for item in cross[max(len(cross) - WINDOW, 0):] + local:
        z_copy(*item).wait_send()
    for d, k in [(0, 0)] + cross + local:
        f_copy(d, k).wait_send()
    for item in cross:
        sent(t_copies(*item))
    waited = range(begun - WINDOW, chunks - WINDOW) if begun < chunks else range(0)
    for h in range(chunks):
        if h not in waited:
            sent(x_copies(h))
        sent(g_copies(h))


def on_device(held, owner_map, kept, left_env, mpo_tensor, mpo_mask, fields):
    envs, cores, planes = (lax.axis_size(name) for name in ("env", "col", "mpo"))
    pool, tile, width = held.shape
    rows, tiles = owner_map.shape
    states = tiles * tile // width
    cap = 2 * kept.shape[0] * tiles // (envs * cores)
    slab = left_env.shape[0]
    slots = slab * planes
    padded = -(-slots // 16) * 16
    share = width // cores
    lanes = -(-share // LANES) * LANES
    chunks = width // ROWS
    bond = mpo_tensor.shape[0]
    list_rows = max(rows, 8) + 8
    smem = pl.BlockSpec(memory_space=pltpu.SMEM)
    vmem = pl.BlockSpec(memory_space=pltpu.VMEM)
    anywhere = pl.BlockSpec(memory_space=pl.ANY)
    dma = pltpu.SemaphoreType.DMA
    assert pool <= 256 and envs & (envs - 1) == 0 and kept.shape[0] == 1

    pieces = PIECES if cap // planes % PIECES == 0 else 1
    result = pl.pallas_call(
        functools.partial(fused_kernel, (envs, planes, cores)),
        out_shape=pltpu.VMEM((slab, share, width), F32),
        in_specs=[smem, smem] + [anywhere] * 5,
        out_specs=vmem,
        scratch_shapes=[
            pltpu.VMEM((pool, tile, width), BF),
            pltpu.VMEM((max(envs - 1, 1), cap, tile, width), BF),
            pltpu.VMEM((envs * cores * cap, tile, width), BF),
            pltpu.VMEM(left_env.shape, BF),
            pltpu.VMEM((slots - slab, width, width), BF),
            pltpu.VMEM((list_rows, tiles), jnp.int32),
            pltpu.SMEM((list_rows, tiles), jnp.int32),
            pltpu.VMEM((bond * states * states, LANES), F32),
            pltpu.VMEM((tiles * tile, width), F32),
            pltpu.VMEM((states, width, lanes), BF),
            pltpu.VMEM((states, ROWS * padded, lanes), BF),
            pltpu.VMEM((slab, ROWS * states, lanes), BF),
            pltpu.VMEM((tiles * tile, width), BF),
            pltpu.VMEM(owner_map.shape, jnp.int32),
            pltpu.VMEM((bond, states, states, bond), F32),
            pltpu.VMEM(mpo_mask.shape, jnp.int32),
            dma((envs, pieces)), dma((envs, pieces)), dma((envs, pieces)), dma((envs, pieces)),
            dma((envs, pieces, planes)), dma((envs, pieces, planes)),
            dma((envs, pieces, planes)), dma((envs, pieces, planes)),
            dma((planes, chunks)), dma((planes, chunks)),
            dma((planes, chunks)), dma((planes, chunks)),
            dma((6,)),
        ],
        compiler_params=pltpu.CompilerParams(
            collective_id=0,
            has_side_effects=True,
            vmem_limit_bytes=62 * 1024 * 1024 - slab * share * width * 4,
        ),
        name="fused",
    )(kept, fields, owner_map, mpo_tensor.transpose(0, 2, 3, 1), mpo_mask, held, left_env)
    return jnp.swapaxes(result, 1, 2)[:, None]


def solution(mesh):
    return jax.shard_map(
        on_device,
        mesh=mesh,
        in_specs=(
            P(("real", "env", "col"), None, None),
            P("real", None),
            P(("real", "env")),
            P("mpo", ("real", "env"), None, None),
            P(),
            P(),
            P("real"),
        ),
        out_specs=P("mpo", ("real", "env"), None, "col"),
        check_vma=False,
    )
```

```python
import functools

import jax
import jax.numpy as jnp
from jax import lax
from jax.experimental import pallas as pl
from jax.experimental.pallas import tpu as pltpu
from jax.sharding import PartitionSpec as P

MESH = pl.DeviceIdType.MESH
LANES = 128
GROUP = 4
STEP = 16
ROWS = 64
EARLY = 3
WINDOW = 2
PIECES = 1
LAG = 2
PREPARE = 1
STRIDE = 2
DELAY = 1
SOLO = 12
BF = jnp.bfloat16
F32 = jnp.float32


def iota(shape, dim):
    return lax.broadcasted_iota(jnp.int32, shape, dim)


def divisor(count, most):
    return max(i for i in range(1, most + 1) if count % i == 0)


def one_hot(condition):
    return jnp.where(condition, F32(1), F32(0)).astype(BF)


def mm(a, b):
    return jnp.dot(a, b, preferred_element_type=F32)


def mm_nt(a, b):
    return lax.dot_general(a, b, (((1,), (1,)), ((), ())), preferred_element_type=F32)


def mm_tn(a, b):
    return lax.dot_general(a, b, (((0,), (0,)), ((), ())), preferred_element_type=F32)


def partner(env, d):
    out = env
    bit = 1
    while bit <= d:
        if d & bit:
            out = out + bit * (1 - 2 * lax.rem(lax.div(env, jnp.int32(bit)), 2))
        bit *= 2
    return out


def plan(envs, planes, cap):
    solo = cap * SOLO // 48
    shareable = planes > 1 and (cap - solo) % (planes * PIECES) == 0
    count = (cap - solo) // (planes * PIECES)
    far = [d for d in range(envs - 1, 0, -1) if d >= envs // 2] if shareable else []
    near = [d for d in range(envs - 1, 0, -1) if d not in far]
    cross, local, at = [], [], 0
    for d in far:
        for k in range(PIECES):
            cross.append((d, solo + k * planes * count, count, True, at))
            at += count
    for d in far:
        if solo:
            cross.append((d, 0, solo, False, at))
            at += solo
    for d in near:
        local.append((d, 0, cap, False, at))
        at += cap
    return cross, local, at


def tile_lists(map_ref, env, me, pool, owners, cap):
    rows, tiles = map_ref.shape
    table = map_ref[...]
    if rows < 8:
        table = jnp.concatenate([table] * (8 // rows), axis=0)
    local = (table - me * pool).astype(F32)
    mine = (local >= 0) & (local < pool)
    earlier = one_hot(iota((tiles, tiles), 0) < iota((tiles, tiles), 1))
    rank = mm(jnp.where(mine, F32(1), F32(0)).astype(BF), earlier)
    key = jnp.where(mine, rank, F32(-1))
    places = rows * cap
    spread = one_hot(
        lax.div(iota((places, table.shape[0]), 0), cap) == iota((places, table.shape[0]), 1)
    )
    place = lax.rem(iota((places, tiles), 0), cap).astype(F32)
    chosen = one_hot(mm(spread, key.astype(BF)) == place)
    send = mm_nt(jnp.where(mine, local, F32(0)).astype(BF), chosen)
    send = send.astype(jnp.int32)

    row = map_ref[pl.ds(env, 1), :].astype(F32)
    owner = jnp.floor((row + 0.5) * F32(1.0 / pool))
    holds = iota((owners, tiles), 0).astype(F32) == owner
    ranks = mm(one_hot(holds), earlier)
    at = owner * cap + jnp.sum(jnp.where(holds, ranks, F32(0)), axis=0, keepdims=True)
    return send, at.astype(jnp.int32)


def mixing_matrix(tensor_ref, mask_ref, fields_ref, table_ref, plane, slab, slots, padded):
    bond, states = tensor_ref.shape[0], tensor_ref.shape[1]
    table_ref[...] = jnp.zeros_like(table_ref)
    lane, state = iota((states, bond), 1), iota((states, bond), 0)
    onsite = fields_ref[0] * (0.5 - lax.div(state, 2).astype(F32)) + fields_ref[1] * (
        0.5 - lax.rem(state, 2).astype(F32)
    )
    for w in range(bond):
        mask = mask_ref[pl.ds(w, 1), :].astype(F32)
        for q in range(states):
            block = tensor_ref[w, q] * mask
            if w == bond - 1:
                block = block + jnp.where((lane == 0) & (state == q), onsite, F32(0))
            table_ref[pl.ds((w * states + q) * states, states), :bond] = block
    table = table_ref[...]
    high = table.astype(BF)
    low = (table - high.astype(F32)).astype(BF)

    wide, tall = states * GROUP * padded, slab * states * GROUP
    entries = table.shape[0]
    at, entry = iota((wide, entries), 0), iota((wide, entries), 1)
    slot = lax.rem(at, padded)
    bond_index = plane * slab + slot
    bond_index = jnp.where(bond_index >= slots, bond_index - slots, bond_index)
    base = bond_index * (states * states) + lax.div(at, GROUP * padded)
    row, col = iota((tall, LANES), 0), iota((tall, LANES), 1)
    unit = states * GROUP
    diagonal = lax.rem(iota((tall, wide), 0), GROUP) == lax.rem(
        lax.div(iota((tall, wide), 1), padded), GROUP
    )
    parts = [jnp.zeros((tall, wide), F32), jnp.zeros((tall, wide), F32)]
    for q in range(states):
        source = one_hot((entry == base + q * states) & (slot < slots))
        target = one_hot(
            (lax.div(lax.rem(row, unit), GROUP) == q) & (col == plane * slab + lax.div(row, unit))
        )
        for i, piece in enumerate((high, low)):
            parts[i] = parts[i] + mm_nt(target, mm(source, piece).astype(BF))
    return jnp.concatenate([jnp.where(diagonal, part, F32(0)).astype(BF) for part in parts], axis=0)


def fused_kernel(
    sizes, kept_ref, fields_ref, map_ref, tensor_ref, mask_ref, held_ref, left_ref,
    out_ref,
    pool_ref, pack_ref, arrived_ref, near_ref, far_ref, vlist_ref, list_ref, table_ref,
    tiles_ref, blocks_ref, own_ref, env_ref, first_ref, second_ref, vmap_ref, vtensor_ref, vmask_ref,
    mixing_ref, interleave_ref, regroup_ref,
    z_sem, f_sem, s_sem, x_sem, local_sem,
):
    envs, planes, cores = sizes
    env, plane, core = lax.axis_index("env"), lax.axis_index("mpo"), lax.axis_index("col")
    pool, tile, width = pool_ref.shape
    rows, tiles = map_ref.shape
    owners = envs * cores
    cap = arrived_ref.shape[0] // owners
    states = tiles * tile // width
    slab = left_ref.shape[0]
    slots = slab * planes
    padded = -(-slots // 16) * 16
    share = width // cores
    mate = lax.rem(core + 1, cores)
    me = env * cores + core
    chunks = width // ROWS
    part = ROWS // cores
    cross, local, _ = plan(envs, planes, cap)
    every = [(0, 0, cap, False, 0)] + cross + local
    last = max([i for i, item in enumerate(cross) if item[3]], default=-1)
    begun = min(EARLY + 2, chunks)
    late = {STRIDE * (c - begun) + DELAY: c for c in range(begun, chunks)}

    barrier = pltpu.get_barrier_semaphore()
    for d in range(1, planes):
        pl.semaphore_signal(
            barrier, inc=1, device_id={"mpo": lax.rem(plane + d, planes)}, device_id_type=MESH
        )
    pl.semaphore_signal(barrier, inc=1, device_id={"col": mate}, device_id_type=MESH)
    for d in range(1, envs):
        pl.semaphore_signal(
            barrier, inc=1, device_id={"env": partner(env, d)}, device_id_type=MESH
        )
    loads = [
        pltpu.make_async_copy(source, target, local_sem.at[i])
        for i, (source, target) in enumerate(
            [
                (map_ref, vmap_ref), (held_ref, pool_ref), (tensor_ref, vtensor_ref),
                (mask_ref, vmask_ref), (left_ref, near_ref), (vlist_ref, list_ref),
            ]
        )
    ]
    for load in loads[:5]:
        load.start()
    loads[0].wait()

    send, at = tile_lists(vmap_ref, env, me, pool, owners, cap)
    send_rows = send.shape[0]
    vlist_ref[:send_rows] = send
    vlist_ref[pl.ds(send_rows, 8)] = jnp.broadcast_to(at, (8, tiles))
    loads[5].start()

    def landed(item, owner_plane, source_env):
        d, first, count, both, _ = item
        if both:
            first = first + owner_plane * count
        return arrived_ref.at[pl.ds((source_env * cores + core) * cap + first, count)]

    def z_copy(item):
        d, first, count, both, place = item
        n = every.index(item)
        return pltpu.make_async_remote_copy(
            src_ref=pack_ref.at[pl.ds(place, count)],
            dst_ref=landed(item, plane, env),
            send_sem=z_sem.at[n - 1, 0], recv_sem=z_sem.at[n - 1, 1],
            device_id={"env": partner(env, d)}, device_id_type=MESH,
        )

    def f_copy(item):
        n = every.index(item)
        block = landed(item, plane, partner(env, item[0]))
        return pltpu.make_async_remote_copy(
            src_ref=block, dst_ref=block,
            send_sem=f_sem.at[n, 0], recv_sem=f_sem.at[n, 1],
            device_id={"col": mate}, device_id_type=MESH,
        )

    def s_copies(item):
        n = cross.index(item)
        block = landed(item, plane, partner(env, item[0]))
        return [
            pltpu.make_async_remote_copy(
                src_ref=block, dst_ref=block,
                send_sem=s_sem.at[n, e - 1, 0], recv_sem=s_sem.at[n, e - 1, 1],
                device_id={"mpo": lax.rem(plane + e, planes)}, device_id_type=MESH,
            )
            for e in range(1, planes)
        ]

    def t_copies(item):
        n = cross.index(item)
        copies = []
        for e in range(1, planes):
            block = landed(item, lax.rem(plane + planes - e, planes), partner(env, item[0]))
            copies.append(
                pltpu.make_async_remote_copy(
                    src_ref=block, dst_ref=block,
                    send_sem=s_sem.at[n, e - 1, 2], recv_sem=s_sem.at[n, e - 1, 3],
                    device_id={"col": mate}, device_id_type=MESH,
                )
            )
        return copies

    def x_copies(h):
        piece = pl.ds(pl.multiple_of(h * ROWS + core * part, part), part)
        return [
            pltpu.make_async_remote_copy(
                src_ref=left_ref.at[:, 0, piece],
                dst_ref=far_ref.at[pl.ds((planes - d - 1) * slab, slab), piece],
                send_sem=x_sem.at[d - 1, h, 0], recv_sem=x_sem.at[d - 1, h, 1],
                device_id={"mpo": lax.rem(plane + d, planes)}, device_id_type=MESH,
            )
            for d in range(1, planes)
        ]

    def g_copies(h):
        piece = pl.ds(pl.multiple_of(h * ROWS + core * part, part), part)
        copies = []
        for d in range(1, planes):
            block = far_ref.at[pl.ds((planes - d - 1) * slab, slab), piece]
            copies.append(
                pltpu.make_async_remote_copy(
                    src_ref=block, dst_ref=block,
                    send_sem=x_sem.at[d - 1, h, 2], recv_sem=x_sem.at[d - 1, h, 3],
                    device_id={"col": mate}, device_id_type=MESH,
                )
            )
        return copies

    def start(copies):
        for copy in copies:
            copy.start()

    def sent(copies):
        for copy in copies:
            copy.wait_send()

    def relay(arrivals, copies):
        for arrival, copy in zip(arrivals, copies):
            arrival.wait_recv()
            copy.start()

    pl.semaphore_wait(barrier, envs + planes - 1)
    for h in range(EARLY):
        start(x_copies(h))
    loads[1].wait()
    loads[5].wait()

    def gather(count, first, store):
        def step(p, carry):
            slot = jnp.clip(list_ref[first[0], first[1] + p], 0, pool - 1)
            store(p, pool_ref[slot])
            return carry

        lax.fori_loop(0, count, step, jnp.int32(0), unroll=divisor(count, 24))

    def pack(item):
        d, first, count, both, place = item
        target = partner(env, d)
        if both:
            first = first + plane * count

        def store(p, value):
            pack_ref[place + p] = value

        gather(count, (target, target * cap + first), store)

    for item in cross[:WINDOW] + local:
        pack(item)
        z_copy(item).start()
    for item in cross[WINDOW:]:
        pack(item)

    def keep(p, value):
        arrived_ref[me * cap + p] = value

    gather(cap, (env, env * cap), keep)
    f_copy(every[0]).start()

    loads[2].wait()
    loads[3].wait()
    mixing_ref[...] = mixing_matrix(
        vtensor_ref, vmask_ref, fields_ref, table_ref, plane, slab, slots, padded
    )
    out_ref[...] = jnp.zeros_like(out_ref)
    unit = states * GROUP
    wide = ROWS * states
    row, col = iota((wide, wide), 0), iota((wide, wide), 1)
    moved = (
        lax.rem(lax.div(row, GROUP), states) * ROWS
        + lax.div(row, unit) * GROUP
        + lax.rem(row, GROUP)
    )
    regroup_ref[...] = one_hot(col == moved)
    block_rows = STEP * padded
    row, col = iota((block_rows, block_rows), 0), iota((block_rows, block_rows), 1)
    interleave_ref[...] = one_hot(col == lax.rem(row, padded) * STEP + lax.div(row, padded))
    loads[4].wait()

    def weave(h, slot):
        for b in range(ROWS // STEP):
            piece = pl.ds(pl.multiple_of(h * ROWS + b * STEP, STEP), STEP)
            stack = [near_ref[w, 0, piece, :] for w in range(slab)]
            stack += [far_ref[w, piece, :] for w in range(slots - slab)]
            if padded > slots:
                stack.append(jnp.zeros(((padded - slots) * STEP, width), BF))
            env_ref[slot, pl.ds(b * block_rows, block_rows)] = mm(
                interleave_ref[...], jnp.concatenate(stack, axis=0)
            ).astype(BF)

    def prepare():
        for h in range(EARLY):
            relay(x_copies(h), g_copies(h))
        for h in range(EARLY):
            for copy in g_copies(h):
                copy.wait_recv()
            weave(h, h)

    def share_in(i):
        if 0 <= i < len(cross) and cross[i][3]:
            relay(s_copies(cross[i]), t_copies(cross[i]))

    def middle():
        for item in cross[: last + 1]:
            sent(s_copies(item))
        for h in range(EARLY, min(EARLY + 2, chunks)):
            start(x_copies(h))

    if last < 0:
        middle()
        prepare()
    for i, item in enumerate(cross):
        if i + WINDOW < len(cross):
            z_copy(item).wait_send()
            z_copy(cross[i + WINDOW]).start()
        z_copy(item).wait_recv()
        if item[3]:
            start(s_copies(item))
        f_copy(item).start()
        share_in(i - LAG)
        if i == min(PREPARE, len(cross) - 1):
            prepare()
        if i == last:
            middle()
    for item in local:
        z_copy(item).wait_recv()
        f_copy(item).start()
    for i in range(max(len(cross) - LAG, 0), len(cross)):
        share_in(i)
    for item in every:
        f_copy(item).wait_recv()
    for item in cross[: last + 1]:
        for copy in t_copies(item):
            copy.wait_recv()

    batch = divisor(tiles, 64)

    def fetch(b, carry):
        for i in range(batch):
            j = b * batch + i
            to = pl.multiple_of(j * tile, tile)
            source = jnp.clip(list_ref[send_rows, j], 0, owners * cap - 1)
            tiles_ref[pl.ds(to, tile), :] = arrived_ref[source].astype(F32)
        return carry

    lax.fori_loop(0, tiles // batch, fetch, jnp.int32(0))

    kept = kept_ref[0]
    first_lane = core * (width - LANES)
    rest = share - LANES
    lane = iota((width, LANES), 1)
    for s in range(states):
        at_rows = pl.ds(s * width, width)
        whole = tiles_ref[at_rows, :]
        blocks_ref[s] = jnp.where(iota((width, width), 1) < kept, whole, F32(0)).astype(BF)
        main = tiles_ref[at_rows, pl.ds(pl.multiple_of(first_lane, LANES), LANES)]
        main = jnp.where(lane + first_lane < kept, main, F32(0))
        own_ref[:, s * LANES : (s + 1) * LANES] = main.astype(BF)
    for p in range(states // 2):
        middles = [
            jnp.where(
                lane + LANES < kept,
                tiles_ref[pl.ds((2 * p + i) * width, width), LANES : 2 * LANES],
                F32(0),
            )
            for i in range(2)
        ]
        left = jnp.where(core == 0, middles[0], pltpu.roll(middles[0], rest, 1))
        right = jnp.where(core == 0, pltpu.roll(middles[1], rest, 1), middles[1])
        at_lanes = (states + p) * LANES
        own_ref[:, at_lanes : at_lanes + LANES] = jnp.where(lane < rest, left, right).astype(BF)

    per_group = GROUP * padded
    tall = slab * states * GROUP
    span = states * per_group
    groups = ROWS // GROUP
    pairs = -(-slab // 2)
    main_rows = pl.ds(pl.multiple_of(core * rest, rest), LANES)
    rest_rows = pl.ds(pl.multiple_of((1 - core) * LANES, rest), rest)

    def mix(operand):
        mixed = mm(mixing_ref[...], operand)
        return mixed[:tall] + mixed[tall:]

    def halves(even, odd):
        low = iota(even.shape, 1) < rest
        return (
            jnp.where(low, even, pltpu.roll(odd, rest, 1)),
            jnp.where(low, pltpu.roll(even, rest, 1), odd),
        )

    def chunk_step(h, carry):
        for when, c in late.items():

            @pl.when(h == when)
            def _(c=c):
                sent(x_copies(c - WINDOW))
                start(x_copies(c))

        @pl.when((h + 1 >= EARLY) & (h + 1 < chunks))
        def _():
            relay(x_copies(h + 1), g_copies(h + 1))


        @pl.when(h >= EARLY)
        def _():
            for copy in g_copies(h):
                copy.wait_recv()
            weave(h, EARLY)

        slot = jnp.minimum(h, EARLY)
        for g in range(0, groups, 2):
            rows_at = pl.ds(g * per_group, 2 * per_group)
            result = mm(env_ref[slot, rows_at], own_ref[...])
            for i in range(2):
                for s in range(states):
                    first_ref[
                        pl.ds((g + i) * span + s * per_group, per_group), :LANES
                    ] = result[i * per_group : (i + 1) * per_group, s * LANES : (s + 1) * LANES].astype(BF)
            for p in range(states // 2):
                at_lanes = (states + p) * LANES
                pair = result[:, at_lanes : at_lanes + LANES]
                for i, piece in enumerate(halves(pair[:per_group], pair[per_group:])):
                    first_ref[
                        pl.ds(g // 2 * span + (2 * p + i) * per_group, per_group), LANES:
                    ] = piece.astype(BF)
        for g in range(0, groups, 2):
            operand = jnp.concatenate(
                [first_ref[pl.ds((g + i) * span, span), :LANES] for i in range(2)], axis=1
            )
            mixed = mix(operand).astype(BF)
            for i in range(2):
                for v in range(slab):
                    second_ref[pl.ds((g + i) * unit, unit), v * LANES : (v + 1) * LANES] = mixed[
                        v * unit : (v + 1) * unit, i * LANES : (i + 1) * LANES
                    ]
        for g in range(0, groups, 4):
            operand = jnp.concatenate(
                [first_ref[pl.ds((g // 2 + i) * span, span), LANES:] for i in range(2)], axis=1
            )
            mixed = mix(operand)
            for i in range(2):
                for p in range(pairs):
                    both = [
                        mixed[
                            min(2 * p + j, slab - 1) * unit : (min(2 * p + j, slab - 1) + 1) * unit,
                            i * LANES : (i + 1) * LANES,
                        ]
                        for j in range(2)
                    ]
                    for j, piece in enumerate(halves(*both)):
                        second_ref[
                            pl.ds((g + 2 * i + j) * unit, unit),
                            (slab + p) * LANES : (slab + p + 1) * LANES,
                        ] = piece.astype(BF)
        stack = jnp.concatenate(
            [blocks_ref[s, pl.ds(pl.multiple_of(h * ROWS, ROWS), ROWS), :] for s in range(states)],
            axis=0,
        )
        right = mm(regroup_ref[...], stack).astype(BF)
        for v in range(slab):
            out_ref[v, main_rows] += mm_tn(second_ref[:, v * LANES : (v + 1) * LANES], right)
        for p in range(pairs):
            at_lanes = (slab + p) * LANES
            closed = mm_tn(second_ref[:, at_lanes : at_lanes + LANES], right)
            out_ref[2 * p, rest_rows] += closed[:rest]
            if 2 * p + 1 < slab:
                out_ref[2 * p + 1, rest_rows] += closed[rest:]
        return carry

    lax.fori_loop(0, chunks, chunk_step, jnp.int32(0))

    for item in cross[max(len(cross) - WINDOW, 0):] + local:
        z_copy(item).wait_send()
    for item in every:
        f_copy(item).wait_send()
    for item in cross[: last + 1]:
        sent(t_copies(item))
    waited = [c - WINDOW for c in late.values()]
    for h in range(chunks):
        if h not in waited:
            sent(x_copies(h))
        sent(g_copies(h))


def on_device(held, owner_map, kept, left_env, mpo_tensor, mpo_mask, fields):
    envs, cores, planes = (lax.axis_size(name) for name in ("env", "col", "mpo"))
    pool, tile, width = held.shape
    rows, tiles = owner_map.shape
    states = tiles * tile // width
    cap = 2 * kept.shape[0] * tiles // (envs * cores)
    slab = left_env.shape[0]
    slots = slab * planes
    padded = -(-slots // 16) * 16
    share = width // cores
    chunks = width // ROWS
    bond = mpo_tensor.shape[0]
    list_rows = max(rows, 8) + 8
    smem = pl.BlockSpec(memory_space=pltpu.SMEM)
    vmem = pl.BlockSpec(memory_space=pltpu.VMEM)
    anywhere = pl.BlockSpec(memory_space=pl.ANY)
    dma = pltpu.SemaphoreType.DMA
    assert share * 2 == 3 * LANES and width == 3 * LANES and pool <= 256 and envs & (envs - 1) == 0 and kept.shape[0] == 1

    cross, local, packed = plan(envs, planes, cap)
    result = pl.pallas_call(
        functools.partial(fused_kernel, (envs, planes, cores)),
        out_shape=pltpu.VMEM((slab, share, width), F32),
        in_specs=[smem, smem] + [anywhere] * 5,
        out_specs=vmem,
        scratch_shapes=[
            pltpu.VMEM((pool, tile, width), BF),
            pltpu.VMEM((packed, tile, width), BF),
            pltpu.VMEM((envs * cores * cap, tile, width), BF),
            pltpu.VMEM(left_env.shape, BF),
            pltpu.VMEM((slots - slab, width, width), BF),
            pltpu.VMEM((list_rows, tiles), jnp.int32),
            pltpu.SMEM((list_rows, tiles), jnp.int32),
            pltpu.VMEM((bond * states * states, LANES), F32),
            pltpu.VMEM((tiles * tile, width), F32),
            pltpu.VMEM((states, width, width), BF),
            pltpu.VMEM((width, states // 2 * 3 * LANES), BF),
            pltpu.VMEM((EARLY + 1, ROWS * padded, width), BF),
            pltpu.VMEM((ROWS * padded * states, 2 * LANES), BF),
            pltpu.VMEM((ROWS * states, (slab + -(-slab // 2)) * LANES), BF),
            pltpu.VMEM(owner_map.shape, jnp.int32),
            pltpu.VMEM((bond, states, states, bond), F32),
            pltpu.VMEM(mpo_mask.shape, jnp.int32),
            pltpu.VMEM((2 * slab * states * GROUP, states * GROUP * padded), BF),
            pltpu.VMEM((STEP * padded, STEP * padded), BF),
            pltpu.VMEM((ROWS * states, ROWS * states), BF),
            dma((len(cross + local), 2)),
            dma((len(cross + local) + 1, 2)),
            dma((max(sum(item[3] for item in cross), 1), max(planes - 1, 1), 4)),
            dma((max(planes - 1, 1), chunks, 4)),
            dma((6,)),
        ],
        compiler_params=pltpu.CompilerParams(
            collective_id=0,
            has_side_effects=True,
            vmem_limit_bytes=62 * 1024 * 1024 - slab * share * width * 4,
        ),
        name="fused",
    )(kept, fields, owner_map, mpo_tensor.transpose(0, 2, 3, 1), mpo_mask, held, left_env)
    return jnp.swapaxes(result, 1, 2)[:, None]


def solution(mesh):
    return jax.shard_map(
        on_device,
        mesh=mesh,
        in_specs=(
            P(("real", "env", "col"), None, None),
            P("real", None),
            P(("real", "env")),
            P("mpo", ("real", "env"), None, None),
            P(),
            P(),
            P("real"),
        ),
        out_specs=P("mpo", ("real", "env"), None, "col"),
        check_vma=False,
    )
```

```python
import functools

import jax
import jax.numpy as jnp
from jax import lax
from jax.experimental import pallas as pl
from jax.experimental.pallas import tpu as pltpu
from jax.sharding import PartitionSpec as P

MESH = pl.DeviceIdType.MESH
LANES = 128
GROUP = 4
STEP = 16
ROWS = 64
EARLY = 3
WINDOW = 2
PIECES = 1
LAG = 2
PREPARE = 1
STRIDE = 2
DELAY = 0
BEGUN = 1
HERE = True
SOLO = 12
BF = jnp.bfloat16
F32 = jnp.float32


def iota(shape, dim):
    return lax.broadcasted_iota(jnp.int32, shape, dim)


def divisor(count, most):
    return max(i for i in range(1, most + 1) if count % i == 0)


def one_hot(condition):
    return jnp.where(condition, F32(1), F32(0)).astype(BF)


def mm(a, b):
    return jnp.dot(a, b, preferred_element_type=F32)


def mm_nt(a, b):
    return lax.dot_general(a, b, (((1,), (1,)), ((), ())), preferred_element_type=F32)


def mm_tn(a, b):
    return lax.dot_general(a, b, (((0,), (0,)), ((), ())), preferred_element_type=F32)


def partner(env, d):
    out = env
    bit = 1
    while bit <= d:
        if d & bit:
            out = out + bit * (1 - 2 * lax.rem(lax.div(env, jnp.int32(bit)), 2))
        bit *= 2
    return out


def plan(envs, planes, cap):
    solo = cap * SOLO // 48
    shareable = planes > 1 and (cap - solo) % (planes * PIECES) == 0
    count = (cap - solo) // (planes * PIECES)
    far = [d for d in range(envs - 1, 0, -1) if d >= envs // 2] if shareable else []
    near = [d for d in range(envs - 1, 0, -1) if d not in far]
    cross, local, at = [], [], 0
    for d in far:
        for k in range(PIECES):
            cross.append((d, solo + k * planes * count, count, True, at))
            at += count
    for d in far:
        if solo:
            cross.append((d, 0, solo, False, at))
            at += solo
    for d in near:
        local.append((d, 0, cap, False, at))
        at += cap
    return cross, local, at


def tile_lists(map_ref, me, pool, cap):
    rows, tiles = map_ref.shape
    table = map_ref[...]
    if rows < 8:
        table = jnp.concatenate([table] * (8 // rows), axis=0)
    local = (table - me * pool).astype(F32)
    mine = (local >= 0) & (local < pool)
    earlier = one_hot(iota((tiles, tiles), 0) < iota((tiles, tiles), 1))
    rank = mm(jnp.where(mine, F32(1), F32(0)).astype(BF), earlier)
    key = jnp.where(mine, rank, F32(-1))
    places = rows * cap
    spread = one_hot(
        lax.div(iota((places, table.shape[0]), 0), cap) == iota((places, table.shape[0]), 1)
    )
    place = lax.rem(iota((places, tiles), 0), cap).astype(F32)
    chosen = one_hot(mm(spread, key.astype(BF)) == place)
    send = mm_nt(jnp.where(mine, local, F32(0)).astype(BF), chosen)
    return send.astype(jnp.int32), earlier


def arrivals(map_ref, env, earlier, pool, owners, cap):
    tiles = map_ref.shape[1]
    row = map_ref[pl.ds(env, 1), :].astype(F32)
    owner = jnp.floor((row + 0.5) * F32(1.0 / pool))
    holds = iota((owners, tiles), 0).astype(F32) == owner
    ranks = mm(one_hot(holds), earlier)
    at = owner * cap + jnp.sum(jnp.where(holds, ranks, F32(0)), axis=0, keepdims=True)
    return at.astype(jnp.int32)


def mixing_matrix(tensor_ref, mask_ref, fields_ref, table_ref, plane, slab, slots, padded):
    bond, states = tensor_ref.shape[0], tensor_ref.shape[1]
    table_ref[...] = jnp.zeros_like(table_ref)
    lane, state = iota((states, bond), 1), iota((states, bond), 0)
    onsite = fields_ref[0] * (0.5 - lax.div(state, 2).astype(F32)) + fields_ref[1] * (
        0.5 - lax.rem(state, 2).astype(F32)
    )
    for w in range(bond):
        mask = mask_ref[pl.ds(w, 1), :].astype(F32)
        for q in range(states):
            block = tensor_ref[w, q] * mask
            if w == bond - 1:
                block = block + jnp.where((lane == 0) & (state == q), onsite, F32(0))
            table_ref[pl.ds((w * states + q) * states, states), :bond] = block
    table = table_ref[...]
    high = table.astype(BF)
    low = (table - high.astype(F32)).astype(BF)

    wide, tall = states * GROUP * padded, slab * states * GROUP
    entries = table.shape[0]
    at, entry = iota((wide, entries), 0), iota((wide, entries), 1)
    slot = lax.rem(at, padded)
    bond_index = plane * slab + slot
    bond_index = jnp.where(bond_index >= slots, bond_index - slots, bond_index)
    base = bond_index * (states * states) + lax.div(at, GROUP * padded)
    row, col = iota((tall, LANES), 0), iota((tall, LANES), 1)
    unit = states * GROUP
    diagonal = lax.rem(iota((tall, wide), 0), GROUP) == lax.rem(
        lax.div(iota((tall, wide), 1), padded), GROUP
    )
    parts = [jnp.zeros((tall, wide), F32), jnp.zeros((tall, wide), F32)]
    for q in range(states):
        source = one_hot((entry == base + q * states) & (slot < slots))
        target = one_hot(
            (lax.div(lax.rem(row, unit), GROUP) == q) & (col == plane * slab + lax.div(row, unit))
        )
        for i, piece in enumerate((high, low)):
            parts[i] = parts[i] + mm_nt(target, mm(source, piece).astype(BF))
    return jnp.concatenate([jnp.where(diagonal, part, F32(0)).astype(BF) for part in parts], axis=0)


def fused_kernel(
    sizes, kept_ref, fields_ref, map_ref, tensor_ref, mask_ref, held_ref, left_ref,
    out_ref,
    pool_ref, pack_ref, arrived_ref, near_ref, far_ref, vlist_ref, list_ref, vsource_ref, source_ref, table_ref,
    tiles_ref, blocks_ref, own_ref, env_ref, first_ref, second_ref, vmap_ref, vtensor_ref, vmask_ref,
    mixing_ref, interleave_ref, regroup_ref,
    z_sem, f_sem, s_sem, x_sem, local_sem,
):
    envs, planes, cores = sizes
    env, plane, core = lax.axis_index("env"), lax.axis_index("mpo"), lax.axis_index("col")
    pool, tile, width = pool_ref.shape
    rows, tiles = map_ref.shape
    owners = envs * cores
    cap = arrived_ref.shape[0] // owners
    states = tiles * tile // width
    slab = left_ref.shape[0]
    slots = slab * planes
    padded = -(-slots // 16) * 16
    share = width // cores
    mate = lax.rem(core + 1, cores)
    me = env * cores + core
    chunks = width // ROWS
    part = ROWS // cores
    cross, local, _ = plan(envs, planes, cap)
    every = [(0, 0, cap, False, 0)] + cross + local
    last = max([i for i, item in enumerate(cross) if item[3]], default=-1)
    begun = min(EARLY + BEGUN, chunks)
    late = {STRIDE * (c - begun) + DELAY: c for c in range(begun, chunks)}

    barrier = pltpu.get_barrier_semaphore()
    for d in range(1, planes):
        pl.semaphore_signal(
            barrier, inc=1, device_id={"mpo": lax.rem(plane + d, planes)}, device_id_type=MESH
        )
    pl.semaphore_signal(barrier, inc=1, device_id={"col": mate}, device_id_type=MESH)
    for d in range(1, envs):
        pl.semaphore_signal(
            barrier, inc=1, device_id={"env": partner(env, d)}, device_id_type=MESH
        )
    loads = [
        pltpu.make_async_copy(source, target, local_sem.at[i])
        for i, (source, target) in enumerate(
            [
                (map_ref, vmap_ref), (held_ref, pool_ref), (tensor_ref, vtensor_ref),
                (mask_ref, vmask_ref), (left_ref, near_ref), (vlist_ref, list_ref),
                (vsource_ref, source_ref),
            ]
        )
    ]
    for load in loads[:5]:
        load.start()
    loads[0].wait()

    send, earlier = tile_lists(vmap_ref, me, pool, cap)
    send_rows = send.shape[0]
    vlist_ref[:send_rows] = send
    loads[5].start()
    vsource_ref[...] = jnp.broadcast_to(
        arrivals(vmap_ref, env, earlier, pool, owners, cap), (8, tiles)
    )
    loads[6].start()

    def landed(item, owner_plane, source_env):
        d, first, count, both, _ = item
        if both:
            first = first + owner_plane * count
        return arrived_ref.at[pl.ds((source_env * cores + core) * cap + first, count)]

    def z_copy(item):
        d, first, count, both, place = item
        n = every.index(item)
        return pltpu.make_async_remote_copy(
            src_ref=pack_ref.at[pl.ds(place, count)],
            dst_ref=landed(item, plane, env),
            send_sem=z_sem.at[n - 1, 0], recv_sem=z_sem.at[n - 1, 1],
            device_id={"env": partner(env, d)}, device_id_type=MESH,
        )

    def f_copy(item):
        n = every.index(item)
        block = landed(item, plane, partner(env, item[0]))
        return pltpu.make_async_remote_copy(
            src_ref=block, dst_ref=block,
            send_sem=f_sem.at[n, 0], recv_sem=f_sem.at[n, 1],
            device_id={"col": mate}, device_id_type=MESH,
        )

    def s_copies(item):
        n = cross.index(item)
        block = landed(item, plane, partner(env, item[0]))
        return [
            pltpu.make_async_remote_copy(
                src_ref=block, dst_ref=block,
                send_sem=s_sem.at[n, e - 1, 0], recv_sem=s_sem.at[n, e - 1, 1],
                device_id={"mpo": lax.rem(plane + e, planes)}, device_id_type=MESH,
            )
            for e in range(1, planes)
        ]

    def t_copies(item):
        n = cross.index(item)
        copies = []
        for e in range(1, planes):
            block = landed(item, lax.rem(plane + planes - e, planes), partner(env, item[0]))
            copies.append(
                pltpu.make_async_remote_copy(
                    src_ref=block, dst_ref=block,
                    send_sem=s_sem.at[n, e - 1, 2], recv_sem=s_sem.at[n, e - 1, 3],
                    device_id={"col": mate}, device_id_type=MESH,
                )
            )
        return copies

    def x_copies(h):
        piece = pl.ds(pl.multiple_of(h * ROWS + core * part, part), part)
        return [
            pltpu.make_async_remote_copy(
                src_ref=left_ref.at[:, 0, piece],
                dst_ref=far_ref.at[pl.ds((planes - d - 1) * slab, slab), piece],
                send_sem=x_sem.at[d - 1, h, 0], recv_sem=x_sem.at[d - 1, h, 1],
                device_id={"mpo": lax.rem(plane + d, planes)}, device_id_type=MESH,
            )
            for d in range(1, planes)
        ]

    def g_copies(h):
        piece = pl.ds(pl.multiple_of(h * ROWS + core * part, part), part)
        copies = []
        for d in range(1, planes):
            block = far_ref.at[pl.ds((planes - d - 1) * slab, slab), piece]
            copies.append(
                pltpu.make_async_remote_copy(
                    src_ref=block, dst_ref=block,
                    send_sem=x_sem.at[d - 1, h, 2], recv_sem=x_sem.at[d - 1, h, 3],
                    device_id={"col": mate}, device_id_type=MESH,
                )
            )
        return copies

    def start(copies):
        for copy in copies:
            copy.start()

    def sent(copies):
        for copy in copies:
            copy.wait_send()

    def relay(arrivals, copies):
        for arrival, copy in zip(arrivals, copies):
            arrival.wait_recv()
            copy.start()

    pl.semaphore_wait(barrier, envs + planes - 1)
    for h in range(EARLY):
        start(x_copies(h))
    loads[1].wait()
    loads[5].wait()

    def gather(count, first, store):
        def step(p, carry):
            slot = jnp.clip(list_ref[first[0], first[1] + p], 0, pool - 1)
            store(p, pool_ref[slot])
            return carry

        lax.fori_loop(0, count, step, jnp.int32(0), unroll=divisor(count, 24))

    def pack(item):
        d, first, count, both, place = item
        target = partner(env, d)
        if both:
            first = first + plane * count

        def store(p, value):
            pack_ref[place + p] = value

        gather(count, (target, target * cap + first), store)

    for item in cross[:WINDOW] + local:
        pack(item)
        z_copy(item).start()
    for item in cross[WINDOW:]:
        pack(item)

    def keep(p, value):
        arrived_ref[me * cap + p] = value

    gather(cap, (env, env * cap), keep)
    f_copy(every[0]).start()

    loads[2].wait()
    loads[3].wait()
    loads[6].wait()
    mixing_ref[...] = mixing_matrix(
        vtensor_ref, vmask_ref, fields_ref, table_ref, plane, slab, slots, padded
    )
    out_ref[...] = jnp.zeros_like(out_ref)
    unit = states * GROUP
    wide = ROWS * states
    row, col = iota((wide, wide), 0), iota((wide, wide), 1)
    moved = (
        lax.rem(lax.div(row, GROUP), states) * ROWS
        + lax.div(row, unit) * GROUP
        + lax.rem(row, GROUP)
    )
    regroup_ref[...] = one_hot(col == moved)
    block_rows = STEP * padded
    row, col = iota((block_rows, block_rows), 0), iota((block_rows, block_rows), 1)
    interleave_ref[...] = one_hot(col == lax.rem(row, padded) * STEP + lax.div(row, padded))
    loads[4].wait()

    def weave(h, slot):
        for b in range(ROWS // STEP):
            piece = pl.ds(pl.multiple_of(h * ROWS + b * STEP, STEP), STEP)
            stack = [near_ref[w, 0, piece, :] for w in range(slab)]
            stack += [far_ref[w, piece, :] for w in range(slots - slab)]
            if padded > slots:
                stack.append(jnp.zeros(((padded - slots) * STEP, width), BF))
            env_ref[slot, pl.ds(b * block_rows, block_rows)] = mm(
                interleave_ref[...], jnp.concatenate(stack, axis=0)
            ).astype(BF)

    def prepare():
        for h in range(EARLY):
            relay(x_copies(h), g_copies(h))
        for h in range(EARLY):
            for copy in g_copies(h):
                copy.wait_recv()
            weave(h, h)

    def share_in(i):
        if 0 <= i < len(cross) and cross[i][3]:
            relay(s_copies(cross[i]), t_copies(cross[i]))

    def near_in():
        for item in local:
            z_copy(item).wait_recv()
            f_copy(item).start()

    def middle():
        for item in cross[: last + 1]:
            sent(s_copies(item))
        for h in range(EARLY, begun):
            start(x_copies(h))

    if last < 0:
        middle()
        prepare()
    for i, item in enumerate(cross):
        if i + WINDOW < len(cross):
            z_copy(item).wait_send()
            z_copy(cross[i + WINDOW]).start()
        z_copy(item).wait_recv()
        if item[3]:
            start(s_copies(item))
        f_copy(item).start()
        share_in(i - LAG)
        if i == min(PREPARE, len(cross) - 1):
            prepare()
        if i == last:
            middle()
            if HERE:
                near_in()
    if last < 0 or not HERE:
        near_in()
    for i in range(max(len(cross) - LAG, 0), len(cross)):
        share_in(i)
    for item in every:
        f_copy(item).wait_recv()
    for item in cross[: last + 1]:
        for copy in t_copies(item):
            copy.wait_recv()

    batch = divisor(tiles, 64)

    def fetch(b, carry):
        for i in range(batch):
            j = b * batch + i
            to = pl.multiple_of(j * tile, tile)
            source = jnp.clip(source_ref[0, j], 0, owners * cap - 1)
            tiles_ref[pl.ds(to, tile), :] = arrived_ref[source].astype(F32)
        return carry

    lax.fori_loop(0, tiles // batch, fetch, jnp.int32(0))

    kept = kept_ref[0]
    first_lane = core * (width - LANES)
    rest = share - LANES
    lane = iota((width, LANES), 1)
    for s in range(states):
        at_rows = pl.ds(s * width, width)
        whole = tiles_ref[at_rows, :]
        blocks_ref[s] = jnp.where(iota((width, width), 1) < kept, whole, F32(0)).astype(BF)
        main = tiles_ref[at_rows, pl.ds(pl.multiple_of(first_lane, LANES), LANES)]
        main = jnp.where(lane + first_lane < kept, main, F32(0))
        own_ref[:, s * LANES : (s + 1) * LANES] = main.astype(BF)
    for p in range(states // 2):
        middles = [
            jnp.where(
                lane + LANES < kept,
                tiles_ref[pl.ds((2 * p + i) * width, width), LANES : 2 * LANES],
                F32(0),
            )
            for i in range(2)
        ]
        left = jnp.where(core == 0, middles[0], pltpu.roll(middles[0], rest, 1))
        right = jnp.where(core == 0, pltpu.roll(middles[1], rest, 1), middles[1])
        at_lanes = (states + p) * LANES
        own_ref[:, at_lanes : at_lanes + LANES] = jnp.where(lane < rest, left, right).astype(BF)

    per_group = GROUP * padded
    tall = slab * states * GROUP
    span = states * per_group
    groups = ROWS // GROUP
    pairs = -(-slab // 2)
    main_rows = pl.ds(pl.multiple_of(core * rest, rest), LANES)
    rest_rows = pl.ds(pl.multiple_of((1 - core) * LANES, rest), rest)

    def mix(operand):
        mixed = mm(mixing_ref[...], operand)
        return mixed[:tall] + mixed[tall:]

    def halves(even, odd):
        low = iota(even.shape, 1) < rest
        return (
            jnp.where(low, even, pltpu.roll(odd, rest, 1)),
            jnp.where(low, pltpu.roll(even, rest, 1), odd),
        )

    def chunk_step(h, carry):
        for when, c in late.items():

            if h == when:
                start(x_copies(c))

        if EARLY <= h + 1 < chunks:
            relay(x_copies(h + 1), g_copies(h + 1))


        if h >= EARLY:
            for copy in g_copies(h):
                copy.wait_recv()
            weave(h, EARLY)

        slot = min(h, EARLY)
        for g in range(0, groups, 2):
            rows_at = pl.ds(g * per_group, 2 * per_group)
            result = mm(env_ref[slot, rows_at], own_ref[...])
            for i in range(2):
                for s in range(states):
                    first_ref[
                        pl.ds((g + i) * span + s * per_group, per_group), :LANES
                    ] = result[i * per_group : (i + 1) * per_group, s * LANES : (s + 1) * LANES].astype(BF)
            for p in range(states // 2):
                at_lanes = (states + p) * LANES
                pair = result[:, at_lanes : at_lanes + LANES]
                for i, piece in enumerate(halves(pair[:per_group], pair[per_group:])):
                    first_ref[
                        pl.ds(g // 2 * span + (2 * p + i) * per_group, per_group), LANES:
                    ] = piece.astype(BF)
        for g in range(0, groups, 2):
            operand = jnp.concatenate(
                [first_ref[pl.ds((g + i) * span, span), :LANES] for i in range(2)], axis=1
            )
            mixed = mix(operand).astype(BF)
            for i in range(2):
                for v in range(slab):
                    second_ref[pl.ds((g + i) * unit, unit), v * LANES : (v + 1) * LANES] = mixed[
                        v * unit : (v + 1) * unit, i * LANES : (i + 1) * LANES
                    ]
        for g in range(0, groups, 4):
            operand = jnp.concatenate(
                [first_ref[pl.ds((g // 2 + i) * span, span), LANES:] for i in range(2)], axis=1
            )
            mixed = mix(operand)
            for i in range(2):
                for p in range(pairs):
                    both = [
                        mixed[
                            min(2 * p + j, slab - 1) * unit : (min(2 * p + j, slab - 1) + 1) * unit,
                            i * LANES : (i + 1) * LANES,
                        ]
                        for j in range(2)
                    ]
                    for j, piece in enumerate(halves(*both)):
                        second_ref[
                            pl.ds((g + 2 * i + j) * unit, unit),
                            (slab + p) * LANES : (slab + p + 1) * LANES,
                        ] = piece.astype(BF)
        stack = jnp.concatenate(
            [blocks_ref[s, pl.ds(pl.multiple_of(h * ROWS, ROWS), ROWS), :] for s in range(states)],
            axis=0,
        )
        right = mm(regroup_ref[...], stack).astype(BF)
        for v in range(slab):
            out_ref[v, main_rows] += mm_tn(second_ref[:, v * LANES : (v + 1) * LANES], right)
        for p in range(pairs):
            at_lanes = (slab + p) * LANES
            closed = mm_tn(second_ref[:, at_lanes : at_lanes + LANES], right)
            out_ref[2 * p, rest_rows] += closed[:rest]
            if 2 * p + 1 < slab:
                out_ref[2 * p + 1, rest_rows] += closed[rest:]
        return carry

    for h in range(chunks):
        chunk_step(h, 0)

    for item in cross[max(len(cross) - WINDOW, 0):] + local:
        z_copy(item).wait_send()
    for item in every:
        f_copy(item).wait_send()
    for item in cross[: last + 1]:
        sent(t_copies(item))
    for h in range(chunks):
        sent(x_copies(h))
        sent(g_copies(h))


def on_device(held, owner_map, kept, left_env, mpo_tensor, mpo_mask, fields):
    envs, cores, planes = (lax.axis_size(name) for name in ("env", "col", "mpo"))
    pool, tile, width = held.shape
    rows, tiles = owner_map.shape
    states = tiles * tile // width
    cap = 2 * kept.shape[0] * tiles // (envs * cores)
    slab = left_env.shape[0]
    slots = slab * planes
    padded = -(-slots // 16) * 16
    share = width // cores
    chunks = width // ROWS
    bond = mpo_tensor.shape[0]
    list_rows = max(rows, 8)
    smem = pl.BlockSpec(memory_space=pltpu.SMEM)
    vmem = pl.BlockSpec(memory_space=pltpu.VMEM)
    anywhere = pl.BlockSpec(memory_space=pl.ANY)
    dma = pltpu.SemaphoreType.DMA
    assert share * 2 == 3 * LANES and width == 3 * LANES and pool <= 256 and envs & (envs - 1) == 0 and kept.shape[0] == 1

    cross, local, packed = plan(envs, planes, cap)
    result = pl.pallas_call(
        functools.partial(fused_kernel, (envs, planes, cores)),
        out_shape=pltpu.VMEM((slab, share, width), F32),
        in_specs=[smem, smem] + [anywhere] * 5,
        out_specs=vmem,
        scratch_shapes=[
            pltpu.VMEM((pool, tile, width), BF),
            pltpu.VMEM((packed, tile, width), BF),
            pltpu.VMEM((envs * cores * cap, tile, width), BF),
            pltpu.VMEM(left_env.shape, BF),
            pltpu.VMEM((slots - slab, width, width), BF),
            pltpu.VMEM((list_rows, tiles), jnp.int32),
            pltpu.SMEM((list_rows, tiles), jnp.int32),
            pltpu.VMEM((8, tiles), jnp.int32),
            pltpu.SMEM((8, tiles), jnp.int32),
            pltpu.VMEM((bond * states * states, LANES), F32),
            pltpu.VMEM((tiles * tile, width), F32),
            pltpu.VMEM((states, width, width), BF),
            pltpu.VMEM((width, states // 2 * 3 * LANES), BF),
            pltpu.VMEM((EARLY + 1, ROWS * padded, width), BF),
            pltpu.VMEM((ROWS * padded * states, 2 * LANES), BF),
            pltpu.VMEM((ROWS * states, (slab + -(-slab // 2)) * LANES), BF),
            pltpu.VMEM(owner_map.shape, jnp.int32),
            pltpu.VMEM((bond, states, states, bond), F32),
            pltpu.VMEM(mpo_mask.shape, jnp.int32),
            pltpu.VMEM((2 * slab * states * GROUP, states * GROUP * padded), BF),
            pltpu.VMEM((STEP * padded, STEP * padded), BF),
            pltpu.VMEM((ROWS * states, ROWS * states), BF),
            dma((len(cross + local), 2)),
            dma((len(cross + local) + 1, 2)),
            dma((max(sum(item[3] for item in cross), 1), max(planes - 1, 1), 4)),
            dma((max(planes - 1, 1), chunks, 4)),
            dma((7,)),
        ],
        compiler_params=pltpu.CompilerParams(
            collective_id=0,
            has_side_effects=True,
            vmem_limit_bytes=62 * 1024 * 1024 - slab * share * width * 4,
        ),
        name="fused",
    )(kept, fields, owner_map, mpo_tensor.transpose(0, 2, 3, 1), mpo_mask, held, left_env)
    return jnp.swapaxes(result, 1, 2)[:, None]


def solution(mesh):
    return jax.shard_map(
        on_device,
        mesh=mesh,
        in_specs=(
            P(("real", "env", "col"), None, None),
            P("real", None),
            P(("real", "env")),
            P("mpo", ("real", "env"), None, None),
            P(),
            P(),
            P("real"),
        ),
        out_specs=P("mpo", ("real", "env"), None, "col"),
        check_vma=False,
    )
```
